32 devices in a mesh: grp: 4 (over y, core), dom: 8 (over z, x).
Axes of the slice: x: 2, y: 2, z: 4, core: 2. Of those that a mesh axis runs over, the one named last changes fastest.
Arguments:
- element_state: float32 [56, 9, 20480], P(None, None, ('grp', 'dom')), may hold values from -6 to 6
- stiffness: float32 [3, 56, 56], replicated, may hold values from -0.75 to 0.75
- flux_local: float32 [4, 56, 56], replicated, may hold values from -0.75 to 0.75
- flux_remote: float32 [4, 56, 56], replicated, may hold values from -0.75 to 0.75
- star_matrix: float32 [3, 9, 9, 20480], P(None, None, None, ('grp', 'dom')), may hold values from -0.18 to 0.18
- face_local: float32 [4, 9, 9, 20480], P(None, None, None, ('grp', 'dom')), may hold values from -0.15 to 0.15
- face_remote: float32 [4, 9, 9, 20480], P(None, None, None, ('grp', 'dom')), may hold values from -0.15 to 0.15
- energy_weight: float32 [9, 20480], P(None, ('grp', 'dom')), may hold values from 0.5 to 18
- face_neighbour: int32 [4, 20480], P(None, ('grp', 'dom')), may hold values from 0 to 1151, as said below
- element_count: int32 [32], P(('grp', 'dom')), may hold values from 160 to 640, as said below
- send_count: int32 [32, 8], P(('grp', 'dom')), may hold values from 0 to 64, as said below
- send_element: int32 [32, 8, 64], P(('grp', 'dom')), may hold values from 0 to 639, as said below
- receiver_element: int32 [512], P(('grp', 'dom')), may hold values from 0 to 639, as said below
- receiver_slot: int32 [512], P(('grp', 'dom')), may hold values from 0 to 127, as said below
- receiver_weight: float32 [56, 512], P(None, ('grp', 'dom')), may hold values from -0.75 to 0.75
Outputs:
- new_state: float32 [56, 9, 20480], P(None, None, ('grp', 'dom'))
- energy: float32 [4, 3], P('grp')
- traces: float32 [3, 9, 512], P(None, None, ('grp', 'dom'))
The draws below stay inside these ranges and needn't reach their ends.
Inputs may be any that keep to these rules, and one draw needn't show every extreme that they name: The first element_count[p] slots of a partition are active. In every slab 4 partitions in a row along dom (cyclically) hold 640 active elements; the others hold from 160 to 320. `send_count`: every partition has exactly 64 in one of its first 6 slots. `send_element`: names active elements of the sending partition. `face_neighbour`: values below 640 name active elements of the partition itself. `receiver_element`: names an active element of the owning partition. `receiver_slot`: within each slab a permutation of the 128 rows.
All inputs are finite; a program needn't handle non-finite values.
Results may differ from the reference program's by a relative error of at most 0.0001.
Values sent between devices are 32-bit elements; how exact they have to be, the bound alone decides.
A program may use at most 128 MiB of HBM per device.

```python
import jax
import jax.numpy as jnp
from jax import lax

BASIS_MODES = 56
QUANTITIES = 9
DIMENSIONS = 3
ELEM_FACES = 4
PEER_REACH = 3
TIME_STEPS = 3
HALO_CAP = 64
ELEM_PAD = 640
REC_DEV = 16
GROUPS = 4
GROUP_SIZE = 8
PARTITIONS = 32
PEER_SLOTS = 8
ELEMENTS = 20480
RECEIVERS = 512


def partition_counts(key):
    base = jax.random.fold_in(key, 101)
    lighter = jax.random.randint(jax.random.fold_in(base, 1), (PARTITIONS,), ELEM_PAD // 4, ELEM_PAD // 2 + 1)
    window = jax.random.randint(jax.random.fold_in(base, 2), (GROUPS,), 0, GROUP_SIZE)
    numbers = jnp.arange(PARTITIONS, dtype=jnp.int32)
    position = (numbers % GROUP_SIZE - window[numbers // GROUP_SIZE]) % GROUP_SIZE
    return jnp.where(position < 4, ELEM_PAD, lighter).astype(jnp.int32)


def draw_element_count(key, part):
    return partition_counts(key)


def draw_send_count(key, part):
    counted = jax.random.randint(jax.random.fold_in(key, 201), (PARTITIONS, PEER_SLOTS), 0, HALO_CAP + 1)
    fullest = jax.random.randint(jax.random.fold_in(key, 202), (PARTITIONS, 1), 0, 2 * PEER_REACH)
    slots_row = jnp.arange(PEER_SLOTS, dtype=jnp.int32)[None, :]
    return jnp.where(slots_row == fullest, HALO_CAP, counted).astype(jnp.int32)


def draw_send_element(key, part):
    counts = partition_counts(key)
    return jax.random.randint(jax.random.fold_in(key, 301), (PARTITIONS, PEER_SLOTS, HALO_CAP), 0, counts[:, None, None]).astype(jnp.int32)


def draw_face_neighbour(key, part):
    counts = partition_counts(key)
    limits = jnp.repeat(counts, ELEM_PAD, total_repeat_length=ELEMENTS)[None, :]
    own_side = jax.random.randint(jax.random.fold_in(key, 401), (ELEM_FACES, ELEMENTS), 0, limits)
    far_side = ELEM_PAD + jax.random.randint(jax.random.fold_in(key, 402), (ELEM_FACES, ELEMENTS), 0, PEER_SLOTS * HALO_CAP)
    chosen = jax.random.randint(jax.random.fold_in(key, 403), (ELEM_FACES, ELEMENTS), 0, 4) == 0
    return jnp.where(chosen, far_side, own_side).astype(jnp.int32)


def draw_receiver_element(key, part):
    counts = partition_counts(key)
    limits = jnp.repeat(counts, REC_DEV, total_repeat_length=RECEIVERS)
    return jax.random.randint(jax.random.fold_in(key, 501), (RECEIVERS,), 0, limits).astype(jnp.int32)


def draw_receiver_slot(key, part):
    group_keys = jax.random.split(jax.random.fold_in(key, 601), GROUPS)
    orders = jax.vmap(lambda group_key: jax.random.permutation(group_key, GROUP_SIZE * REC_DEV))(group_keys)
    return orders.reshape(-1).astype(jnp.int32)


def draw_energy_weight(key, part):
    uniform_part = jax.random.uniform(jax.random.fold_in(key, 701), (QUANTITIES, ELEMENTS), jnp.float32)
    position = (jnp.arange(ELEMENTS, dtype=jnp.int32) // ELEM_PAD % GROUP_SIZE).astype(jnp.float32)
    rising = 1.0 + 2.0 * position / (GROUP_SIZE - 1)
    return (jnp.exp(jnp.log(0.5) + uniform_part * jnp.log(4.0)) * rising).astype(jnp.float32)


def level_of(key, shape, cuts, low, largest):
    gain = 1.0
    for axis_at, blocks in cuts:
        draws = jax.random.uniform(jax.random.fold_in(jax.random.fold_in(key, 6), axis_at), (blocks,), jnp.float32, low / len(cuts), largest / len(cuts))
        gain = gain * jnp.repeat(jnp.exp(draws), shape[axis_at] // blocks).reshape((-1,) + (1,) * (len(shape) - 1 - axis_at))
    return gain


def normal_values(rng, shape, deviation, bound, cuts=(), kind=jnp.bfloat16):
    result = deviation * jax.random.normal(rng, shape, jnp.float32)
    if cuts:
        result = result * level_of(rng, shape, cuts, -0.22, 0.18)
    return jnp.clip(result, -bound, bound).astype(kind)


def setup_inputs(seed: int = 0) -> dict:
    arg_keys = jax.random.split(jax.random.key(seed), 16)
    element_state = normal_values(arg_keys[0], (BASIS_MODES, QUANTITIES, ELEMENTS), 1.0, 6.0, ((2, 32),), jnp.float32)
    stiffness = normal_values(arg_keys[1], (DIMENSIONS, BASIS_MODES, BASIS_MODES), BASIS_MODES ** -0.5, 0.75, (), jnp.float32)
    flux_local = normal_values(arg_keys[2], (ELEM_FACES, BASIS_MODES, BASIS_MODES), BASIS_MODES ** -0.5, 0.75, (), jnp.float32)
    flux_remote = normal_values(arg_keys[3], (ELEM_FACES, BASIS_MODES, BASIS_MODES), BASIS_MODES ** -0.5, 0.75, (), jnp.float32)
    star_matrix = normal_values(arg_keys[4], (DIMENSIONS, QUANTITIES, QUANTITIES, ELEMENTS), 0.03, 0.18, ((3, 32),), jnp.float32)
    face_local = normal_values(arg_keys[5], (ELEM_FACES, QUANTITIES, QUANTITIES, ELEMENTS), 0.025, 0.15, ((3, 32),), jnp.float32)
    face_remote = normal_values(arg_keys[6], (ELEM_FACES, QUANTITIES, QUANTITIES, ELEMENTS), 0.025, 0.15, ((3, 32),), jnp.float32)
    energy_weight = draw_energy_weight(jax.random.fold_in(arg_keys[15], 71), 0)
    face_neighbour = draw_face_neighbour(jax.random.fold_in(arg_keys[15], 71), 0)
    element_count = draw_element_count(jax.random.fold_in(arg_keys[15], 71), 0)
    send_count = draw_send_count(jax.random.fold_in(arg_keys[15], 71), 0)
    send_element = draw_send_element(jax.random.fold_in(arg_keys[15], 71), 0)
    receiver_element = draw_receiver_element(jax.random.fold_in(arg_keys[15], 71), 0)
    receiver_slot = draw_receiver_slot(jax.random.fold_in(arg_keys[15], 71), 0)
    receiver_weight = normal_values(arg_keys[14], (BASIS_MODES, RECEIVERS), BASIS_MODES ** -0.5, 0.75, ((1, 32),), jnp.float32)
    return dict(element_state=element_state, stiffness=stiffness, flux_local=flux_local, flux_remote=flux_remote, star_matrix=star_matrix, face_local=face_local, face_remote=face_remote, energy_weight=energy_weight, face_neighbour=face_neighbour, element_count=element_count, send_count=send_count, send_element=send_element, receiver_element=receiver_element, receiver_slot=receiver_slot, receiver_weight=receiver_weight)


highest = lax.Precision.HIGHEST


def modal(matrix, field):
    flat = field.reshape(field.shape[0], -1)
    product = jnp.dot(matrix, flat, precision=highest, preferred_element_type=jnp.float32)
    return product.reshape((matrix.shape[0],) + field.shape[1:])


def quantity_map(matrices, field):
    return jnp.einsum("pqe,bqe->bpe", matrices, field, precision=highest)


def per_partition(array):
    shaped = array.reshape(array.shape[:-1] + (PARTITIONS, ELEM_PAD))
    return jnp.moveaxis(shaped, -2, 0)


def slot_offset(slot_number):
    if slot_number < PEER_REACH:
        return slot_number + 1
    if slot_number < 2 * PEER_REACH:
        return PEER_REACH - 1 - slot_number
    if slot_number == 2 * PEER_REACH:
        return 1
    return -1


def reference(element_state, stiffness, flux_local, flux_remote, star_matrix, face_local, face_remote, energy_weight, face_neighbour, element_count, send_count, send_element, receiver_element, receiver_slot, receiver_weight):
    fields = per_partition(element_state)
    stars = per_partition(star_matrix)
    local_faces = per_partition(face_local)
    remote_faces = per_partition(face_remote)
    weights = per_partition(energy_weight)
    neighbours = per_partition(face_neighbour)
    receiver_rows = jnp.moveaxis(receiver_weight.reshape(BASIS_MODES, PARTITIONS, REC_DEV), 1, 0)
    receiver_cells = receiver_element.reshape(PARTITIONS, REC_DEV)
    numbers = jnp.arange(PARTITIONS, dtype=jnp.int32)
    group_of = numbers // GROUP_SIZE
    place_of = numbers % GROUP_SIZE
    source_list = []
    present_list = []
    for slot_number in range(PEER_SLOTS):
        offset = slot_offset(slot_number)
        if slot_number < 2 * PEER_REACH:
            source_list.append(group_of * GROUP_SIZE + (place_of - offset) % GROUP_SIZE)
            present_list.append(jnp.ones((PARTITIONS,), dtype=bool))
        else:
            other = group_of - offset
            present_list.append((other >= 0) & (other < GROUPS))
            source_list.append(jnp.clip(other, 0, GROUPS - 1) * GROUP_SIZE + place_of)
    sources = jnp.stack(source_list, 1).astype(jnp.int32)
    present = jnp.stack(present_list, 1)
    live_mask = jnp.arange(ELEM_PAD, dtype=jnp.int32)[None, :] < element_count[:, None]
    slot_live = jnp.arange(HALO_CAP, dtype=jnp.int32)[None, None, :] < send_count[:, :, None]
    denominator = GROUP_SIZE * ELEM_PAD * BASIS_MODES * QUANTITIES
    global_slot = ((jnp.arange(RECEIVERS, dtype=jnp.int32) // (GROUP_SIZE * REC_DEV)) * (GROUP_SIZE * REC_DEV) + receiver_slot).astype(jnp.int32)

    def pack(field, elements, live):
        taken = jnp.take(field, elements, axis=2)
        return jnp.where(live[None, None], taken, jnp.float32(0.0))

    def advance(fields):
        messages = jax.vmap(pack)(fields, send_element, slot_live)

        def update_one(items):
            field, star_here, local_here, remote_here, neighbour_here, source_here, present_here, live_here = items
            pieces = []
            for slot_number in range(PEER_SLOTS):
                sent = lax.dynamic_index_in_dim(messages, source_here[slot_number], 0, keepdims=False)[:, :, slot_number, :]
                pieces.append(jnp.where(present_here[slot_number], sent, jnp.float32(0.0)))
            halo = jnp.stack(pieces, 2).reshape(BASIS_MODES, QUANTITIES, PEER_SLOTS * HALO_CAP)
            extended = jnp.concatenate([field, halo], 2)
            change = jnp.zeros(field.shape, jnp.float32)
            for dimension in range(DIMENSIONS):
                change = change + quantity_map(star_here[dimension], modal(stiffness[dimension], field))
            for face_number in range(ELEM_FACES):
                change = change - quantity_map(local_here[face_number], modal(flux_local[face_number], field))
                nearby = jnp.take(extended, neighbour_here[face_number], axis=2)
                change = change - quantity_map(remote_here[face_number], modal(flux_remote[face_number], nearby))
            return jnp.where(live_here[None, None, :], field + change, field)

        return lax.map(update_one, (fields, stars, local_faces, remote_faces, neighbours, sources, present, live_mask))

    energies = []
    tables = []
    for time_step in range(TIME_STEPS):
        fields = advance(fields)
        squares = jnp.sum(fields * fields, axis=1)
        terms = 0.5 * jnp.sum(jnp.where(live_mask[:, None, :], weights * squares, jnp.float32(0.0)), axis=(1, 2))
        energies.append(terms.reshape(GROUPS, GROUP_SIZE).sum(1) / denominator)

        def sample(field, elements, rows_here):
            return jnp.einsum("br,bqr->qr", rows_here, jnp.take(field, elements, axis=2), precision=highest)

        values = jax.vmap(sample)(fields, receiver_cells, receiver_rows)
        flat = jnp.moveaxis(values, 0, 1).reshape(QUANTITIES, RECEIVERS)
        tables.append(jnp.zeros((QUANTITIES, RECEIVERS), jnp.float32).at[:, global_slot].set(flat))
    new_state = jnp.moveaxis(fields, 0, 2).reshape(BASIS_MODES, QUANTITIES, ELEMENTS)
    return new_state, jnp.stack(energies, 1), jnp.stack(tables, 0)
```

```python
import functools

import jax
import jax.numpy as jnp
from jax import lax
from jax.experimental import pallas as pl
from jax.experimental.pallas import tpu as pltpu
from jax.sharding import PartitionSpec as P

PEER_REACH = 3
TIME_STEPS = 3
LANES = 128
NEAR = (0, PEER_REACH, 2 * PEER_REACH, 2 * PEER_REACH + 1)
FAR = tuple(s for n in range(1, PEER_REACH) for s in (n, PEER_REACH + n))
ORDER = NEAR + FAR
MESH = pl.DeviceIdType.MESH
f32, bf16 = jnp.float32, jnp.bfloat16


def dot(a, b):
    return jnp.dot(a, b, preferred_element_type=f32)


def halves(field):
    high = field.astype(bf16)
    return high, (field - high.astype(f32)).astype(bf16)


def stacked_rows(field):
    high = field.astype(bf16).astype(f32)
    both = jnp.concatenate([high, field - high], 0).astype(bf16)
    return jnp.concatenate([both, both], 0)


def stacked_matrix(matrices):
    high = lax.reduce_precision(matrices, 8, 7)
    low = (matrices - high).astype(bf16)
    high = high.astype(bf16)
    return jnp.concatenate([high, high, low, low], 2)


def row_chunks(rows):
    middle = min(rows, 32)
    return [(0, middle), (middle, rows)] if middle < rows else [(0, rows)]


def halo_ways(slot_number):
    if slot_number < PEER_REACH:
        return "dom", slot_number + 1
    if slot_number < 2 * PEER_REACH:
        return "dom", PEER_REACH - 1 - slot_number
    return "grp", 1 if slot_number == 2 * PEER_REACH else -1


def peer(axis, by):
    place = lax.axis_index(axis)
    count = lax.axis_size(axis)
    if axis == "dom":
        return {axis: lax.rem(place + by + count, count)}, None
    other = place + by
    return {axis: jnp.clip(other, 0, count - 1)}, (other >= 0) & (other < count)


def guarded(condition, action):
    if condition is None:
        action()
    else:
        pl.when(condition)(action)


def hot_of(first, rows, names):
    place = lax.broadcasted_iota(jnp.int32, (rows, names.shape[1]), 0) + first
    return jnp.where(place == names, 1.0, 0.0).astype(bf16)


def steps_kernel(
    x_hbm, star_hbm, near_hbm, far_hbm,
    mats_ref, weight_ref, faces_ref, names_ref, gains_ref, recs_ref, count_ref,
    out_ref, energy_ref, trace_ref,
    star_ref, near_ref, far_ref, both, cat, terms, part, tcat, rterm, hs, th,
    hot_own, hot_halo, hot_up, hot_low, hot_rec, msg, held, mine, tabs,
    load_sem, send_sem, recv_sem, table_send, table_recv,
):
    quantities, basis, elements = out_ref.shape
    rows = quantities * basis
    slots = msg.shape[0]
    half = LANES // 2
    upper = msg.shape[1]
    lower = rows - upper
    faces = far_ref.shape[2]
    dims = star_ref.shape[2]
    own_rows = (dims + faces) * basis
    group = slots // 2 * half
    steps = TIME_STEPS
    size = lax.axis_size("dom")
    me = lax.axis_index("dom")
    receivers = trace_ref.shape[2]
    ways = [halo_ways(slot) for slot in range(slots)]

    barrier = pltpu.get_barrier_semaphore()

    def dom_other(step):
        return {"dom": lax.rem(me + step, size)}

    def greet(step, carry):
        pl.semaphore_signal(barrier, inc=1, device_id=dom_other(step), device_id_type=MESH)
        return carry

    lax.fori_loop(1, size, greet, 0)
    greeted = size - 1
    for axis, by in ways:
        if axis == "grp":
            device, there = peer(axis, by)
            guarded(
                there,
                functools.partial(pl.semaphore_signal, barrier, inc=1, device_id=device, device_id_type=MESH),
            )
            greeted = greeted + there.astype(jnp.int32)

    loads = [
        pltpu.make_async_copy(source, target, load_sem.at[n])
        for n, (source, target) in enumerate(
            [(x_hbm, out_ref), (star_hbm, star_ref), (near_hbm, near_ref), (far_hbm, far_ref)]
        )
    ]
    for load in loads:
        load.start()

    def copy(step, slot):
        device, there = peer(*ways[slot])
        return (
            pltpu.make_async_remote_copy(
                src_ref=msg.at[slot],
                dst_ref=held.at[step, slot],
                send_sem=send_sem.at[step, slot],
                recv_sem=recv_sem.at[step, slot],
                device_id=device,
                device_id_type=MESH,
            ),
            there,
        )

    def start_slots(step, some):
        for slot in some:
            sent, there = copy(step, slot)
            guarded(there, sent.start)

    def wait_slots(step, some):
        for slot in some:
            sent, _ = copy(step, slot)
            axis, by = ways[slot]
            _, came = peer(axis, -by)
            guarded(came, sent.wait_recv)

    for slot in range(slots):
        axis, by = ways[slot]
        _, came = peer(axis, -by)
        if came is not None:

            @pl.when(jnp.logical_not(came))
            def _(slot=slot):
                for step in range(steps):
                    held[step, slot] = jnp.zeros(held.shape[2:], f32)

    width = 2 * LANES
    for pair in range(slots // 2):
        even, odd = ORDER[2 * pair], ORDER[2 * pair + 1]
        first, second = names_ref[even : even + 1, :], names_ref[odd : odd + 1, :]
        tile = slice(pair * LANES, (pair + 1) * LANES)
        straight = hot_of(0, elements, jnp.concatenate([first, second], 1))
        crossed = hot_of(0, elements, jnp.concatenate([second, first], 1))
        for again in range(2):
            hot_up[again * elements : (again + 1) * elements, tile] = straight
            hot_low[again * elements : (again + 1) * elements, tile] = crossed

    def paired(action):
        def one(i, carry):
            action(2 * i, 2)
            return carry

        lax.fori_loop(0, quantities // 2, one, 0)
        if quantities % 2:
            action(quantities - 1, 1)

    def split(q, count):
        field = jnp.concatenate([out_ref[q + n] for n in range(count)], 0)
        high, low = halves(field)
        at = pl.ds(pl.multiple_of(q * basis, 16) if not isinstance(q, int) else q * basis, count * basis)
        cat[at, :elements] = high
        cat[at, elements:] = low

    lane = lax.broadcasted_iota(jnp.int32, (upper, LANES), 1)

    def pack(number):
        lanes = slice(number * width, (number + 1) * width)
        up = dot(cat[:upper, :], hot_up[:, lanes])
        low = dot(cat[upper:rows, :], hot_low[:, lanes])
        for pair in range(width // LANES):
            tile = slice(pair * LANES, (pair + 1) * LANES)
            even, odd = ORDER[number * 4 + 2 * pair], ORDER[number * 4 + 2 * pair + 1]
            top, bottom = up[:, tile], low[:, tile]
            here = lane[:lower]
            msg[even, :lower, :] = jnp.where(here < half, top[:lower], bottom)
            msg[odd, :lower, :] = jnp.where(here < half, bottom, top[:lower])
            msg[even, lower:, :] = top[lower:]
            msg[odd, lower:, :] = top[lower:]

    def pack_and_send(step):
        pack(0)
        start_slots(step, NEAR)
        pack(1)
        start_slots(step, FAR)

    loads[0].wait()
    paired(split)
    pl.semaphore_wait(barrier, greeted)
    pack_and_send(0)

    for f in range(faces):
        names = faces_ref[f : f + 1, :]
        own = hot_of(0, elements, names)
        hot_own[f, :elements, :] = own
        hot_own[f, elements:, :] = own
        for g in range(2):
            for n in range(slots // 2):
                some = hot_of(elements + ORDER[g * (slots // 2) + n] * half, half, names)
                hot_halo[g * faces + f, n * half : (n + 1) * half, :] = some
                hot_halo[g * faces + f, group + n * half : group + (n + 1) * half, :] = some
    hot = hot_of(0, elements, recs_ref[0:1, :])
    hot_rec[:elements, :] = hot
    hot_rec[elements:, :] = hot
    lane_row = lax.broadcasted_iota(jnp.int32, (1, elements), 1)
    live = lane_row < count_ref[0]
    for load in loads[1:]:
        load.wait()

    def store_split(ref, f, q, count, parts, at, gap):
        high, low = halves(jnp.concatenate(parts, 0) if count > 1 else parts[0])
        where = pl.ds(pl.multiple_of(q * basis, 16) if not isinstance(q, int) else q * basis, count * basis)
        wide = high.shape[1]
        ref[f, where, pl.ds(at, wide)] = high
        ref[f, where, pl.ds(at + gap, wide)] = low

    def local_block(at, wide):
        def products(q, count):
            results = [dot(mats_ref[...], both[q + n, :, pl.ds(at, wide)]) for n in range(count)]
            for n in range(count):
                terms[q + n, :, :wide] = results[n][:own_rows]
            for f in range(faces):
                low = own_rows + f * basis
                store_split(tcat, f, q, count, [r[low : low + basis] for r in results], at, elements)

        paired(products)
        for sub in range(wide // LANES):
            lanes = pl.ds(at + sub * LANES, LANES)
            tile = slice(sub * LANES, (sub + 1) * LANES)
            for first, last in row_chunks(basis):

                def one_quantity(q, sums):
                    for n in range(dims + faces):
                        ref, k = (star_ref, n) if n < dims else (near_ref, n - dims)
                        term = terms[q, n * basis + first : n * basis + last, tile]
                        sums = sums + ref[:, q, k : k + 1, lanes] * term[None]
                    return sums

                start = jnp.zeros((quantities, last - first, LANES), f32)
                part[:, first:last, lanes] = lax.fori_loop(0, quantities, one_quantity, start)

    def own_face(f, carry):
        rterm[f] = dot(tcat[f], hot_own[f])
        return carry

    def halo_group(step, g):
        for pair in range(slots // 4):
            tile = slice(pair * LANES, (pair + 1) * LANES)
            at = g * (slots // 2) + 2 * pair
            even, odd = held[step, ORDER[at]], held[step, ORDER[at + 1]]
            hs[:upper, tile] = jnp.where(lane < half, even, odd)
            hs[upper:, tile] = pltpu.roll(jnp.where(lane < half, odd, even), half, 1)[: hs.shape[0] - upper]

        def products(q, count):
            results = []
            for n in range(count):
                start = (q + n) * basis
                start = start if isinstance(start, int) else pl.multiple_of(start, 8)
                results.append(dot(mats_ref[own_rows:, :], stacked_rows(hs[pl.ds(start, basis), :])))
            for f in range(faces):
                store_split(th, f, q, count, [r[f * basis : (f + 1) * basis] for r in results], 0, group)

        paired(products)

        def one_face(f, carry):
            rterm[f] = rterm[f] + dot(th[f], hot_halo[g * faces + f])
            return carry

        lax.fori_loop(0, faces, one_face, 0)

    def finish_block(number, carry):
        lanes = pl.ds(pl.multiple_of(number * LANES, LANES), LANES)
        alive = number * LANES + lax.broadcasted_iota(jnp.int32, (1, LANES), 1) < count_ref[0]
        for first, last in row_chunks(basis):

            def one_quantity(q, sums):
                for f in range(faces):
                    start = pl.multiple_of(q * basis + first, 8)
                    term = rterm[f, pl.ds(start, last - first), lanes]
                    sums = sums + far_ref[:, q, f : f + 1, lanes] * term[None]
                return sums

            sums = lax.fori_loop(0, quantities, one_quantity, part[:, first:last, lanes])
            field = out_ref[:, first:last, lanes]
            out_ref[:, first:last, lanes] = jnp.where(alive[None], field + sums, field)
        return carry

    def table_copy(step, by, source):
        return pltpu.make_async_remote_copy(
            src_ref=mine.at[step],
            dst_ref=tabs.at[step, source],
            send_sem=table_send.at[step, by],
            recv_sem=table_recv.at[step, source],
            device_id=dom_other(by),
            device_id_type=MESH,
        )

    def one_step(step, carry):
        for q in range(quantities):
            both[q] = stacked_rows(out_ref[q])
        at = 0
        while at < elements:
            wide = min(width, elements - at)
            local_block(at, wide)
            at += wide
        lax.fori_loop(0, faces, own_face, 0)
        wait_slots(step, NEAR)
        halo_group(step, 0)
        wait_slots(step, FAR)
        halo_group(step, 1)
        lax.fori_loop(0, elements // LANES, finish_block, 0)
        paired(split)
        for slot in range(slots):
            sent, there = copy(step, slot)
            guarded(there, sent.wait_send)

        @pl.when(step + 1 < steps)
        def _():
            pack_and_send(step + 1)

        total = jnp.zeros((1, elements), f32)
        picked = dot(cat[...], hot_rec[...])
        for q in range(quantities):
            field = out_ref[q]
            total = total + gains_ref[q : q + 1, :] * jnp.sum(field * field, axis=0, keepdims=True)
            here = picked[q * basis : (q + 1) * basis] * weight_ref[...]
            mine[step, q : q + 1, :] = jnp.sum(here, axis=0, keepdims=True)
        total = jnp.where(live, total, 0.0)
        folded = total[:, :LANES]
        for n in range(1, elements // LANES):
            folded = folded + total[:, n * LANES : (n + 1) * LANES]
        mine[step, quantities : quantities + 1, :] = folded
        mine[step, quantities + 1 : quantities + 2, :] = recs_ref[1:2, :].astype(f32)

        def start(by, carry):
            table_copy(step, by, me).start()
            return carry

        lax.fori_loop(1, size, start, 0)
        tabs[step, me] = mine[step]
        return carry

    unused = mine.shape[1] - quantities - 2
    for step in range(steps):
        mine[step, quantities + 2 :, :] = jnp.zeros((unused, LANES), f32)
    lax.fori_loop(0, steps, one_step, 0)

    for step in range(steps):

        def finish(by, carry):
            table_copy(step, by, me).wait_send()
            table_copy(step, by, lax.rem(me + by, size)).wait_recv()
            return carry

        lax.fori_loop(1, size, finish, 0)
    wanted = (me * receivers + lax.broadcasted_iota(jnp.int32, (receivers, LANES), 0)).astype(f32)
    hits, values = [], []
    for source in range(size):
        slot_row = tabs[0, source, quantities + 1 : quantities + 2, :]
        hits.append(jnp.where(wanted == slot_row, 1.0, 0.0).astype(bf16))
        values.append(jnp.concatenate([tabs[step, source] for step in range(steps)], 0))
    hit = jnp.concatenate(hits, 1)
    value = jnp.concatenate(values, 1)
    contract = (((1,), (1,)), ((), ()))
    result = 0.0
    for piece in halves(value):
        result = result + lax.dot_general(piece, hit, contract, preferred_element_type=f32)
    deep = mine.shape[1]
    denominator = float(size * elements * basis * quantities)
    for step in range(steps):
        for q in range(quantities):
            trace_ref[q, step : step + 1, :] = result[step * deep + q : step * deep + q + 1, :]
        row = tabs[step, 0, quantities : quantities + 1, :]
        for source in range(1, size):
            row = row + tabs[step, source, quantities : quantities + 1, :]
        energy_ref[0:1, step : step + 1] = jnp.sum(row, axis=1, keepdims=True) * (0.5 / denominator)


def per_device(
    element_state,
    stiffness,
    flux_local,
    flux_remote,
    star_matrix,
    face_local,
    face_remote,
    energy_weight,
    face_neighbour,
    element_count,
    send_count,
    send_element,
    receiver_element,
    receiver_slot,
    receiver_weight,
):
    basis, quantities, elements = element_state.shape
    slots, capacity = send_element.shape[1:]
    receivers = receiver_slot.shape[0]
    dimensions, faces = stiffness.shape[0], flux_local.shape[0]
    size = lax.axis_size("dom")
    rows = quantities * basis
    upper = (rows // 2 + 15) // 16 * 16
    group = slots // 2 * capacity
    deep = (quantities + 2 + 7) // 8 * 8

    mats = stacked_matrix(jnp.concatenate([stiffness, -flux_local, -flux_remote], 0))
    mats = mats.reshape(-1, mats.shape[2])
    slot_live = jnp.arange(capacity)[None, :] < send_count[0][:, None]
    names = jnp.where(slot_live, send_element[0], -1)
    recs = jnp.pad(
        jnp.stack([receiver_element, receiver_slot]), ((0, 0), (0, LANES - receivers)), constant_values=-1
    )
    rec_weight = jnp.pad(receiver_weight, ((0, 0), (0, LANES - receivers)))
    fields = jnp.transpose(element_state, (1, 0, 2))
    stars = jnp.transpose(star_matrix, (1, 2, 0, 3))
    near = jnp.transpose(face_local, (1, 2, 0, 3))
    far = jnp.transpose(face_remote, (1, 2, 0, 3))

    in_vmem = pl.BlockSpec(memory_space=pltpu.VMEM)
    in_hbm = pl.BlockSpec(memory_space=pltpu.HBM)
    in_smem = pl.BlockSpec(memory_space=pltpu.SMEM)
    vmem = pltpu.VMEM
    state, energy, traces = pl.pallas_call(
        steps_kernel,
        out_shape=(
            jax.ShapeDtypeStruct((quantities, basis, elements), f32),
            jax.ShapeDtypeStruct((1, TIME_STEPS), f32),
            jax.ShapeDtypeStruct((quantities, TIME_STEPS, receivers), f32),
        ),
        in_specs=[in_hbm] * 4 + [in_vmem] * 6 + [in_smem],
        out_specs=(in_vmem,) * 3,
        scratch_shapes=[
            vmem(stars.shape, f32),
            vmem(near.shape, f32),
            vmem(far.shape, f32),
            vmem((quantities, 4 * basis, elements), bf16),
            vmem((rows, 2 * elements), bf16),
            vmem((quantities, (dimensions + faces) * basis, 2 * LANES), f32),
            vmem((quantities, basis, elements), f32),
            vmem((faces, rows, 2 * elements), bf16),
            vmem((faces, rows, elements), f32),
            vmem((rows, group), f32),
            vmem((faces, rows, 2 * group), bf16),
            vmem((faces, 2 * elements, elements), bf16),
            vmem((2 * faces, 2 * group, elements), bf16),
            vmem((2 * elements, slots * capacity), bf16),
            vmem((2 * elements, slots * capacity), bf16),
            vmem((2 * elements, LANES), bf16),
            vmem((slots, upper, LANES), f32),
            vmem((TIME_STEPS, slots, upper, LANES), f32),
            vmem((TIME_STEPS, deep, LANES), f32),
            vmem((TIME_STEPS, size, deep, LANES), f32),
            pltpu.SemaphoreType.DMA((4,)),
            pltpu.SemaphoreType.DMA((TIME_STEPS, slots)),
            pltpu.SemaphoreType.DMA((TIME_STEPS, slots)),
            pltpu.SemaphoreType.DMA((TIME_STEPS, size)),
            pltpu.SemaphoreType.DMA((TIME_STEPS, size)),
        ],
        compiler_params=pltpu.CompilerParams(
            vmem_limit_bytes=60 << 20, collective_id=0, has_side_effects=True
        ),
        name="steps",
    )(
        fields, stars, near, far,
        mats, rec_weight, face_neighbour, names, energy_weight, recs, element_count,
    )
    return (
        jnp.transpose(state, (1, 0, 2)),
        energy,
        jnp.transpose(traces, (1, 0, 2)),
    )


def solution(mesh):
    both = ("grp", "dom")
    return jax.shard_map(
        per_device,
        mesh=mesh,
        in_specs=(
            P(None, None, both),
            P(),
            P(),
            P(),
            P(None, None, None, both),
            P(None, None, None, both),
            P(None, None, None, both),
            P(None, both),
            P(None, both),
            P(both),
            P(both, None),
            P(both, None, None),
            P(both),
            P(both),
            P(None, both),
        ),
        out_specs=(P(None, None, both), P("grp", None), P(None, None, both)),
        check_vma=False,
    )
```

```python
import functools

import jax
import jax.numpy as jnp
from jax import lax
from jax.experimental import pallas as pl
from jax.experimental.pallas import tpu as pltpu
from jax.sharding import PartitionSpec as P

PEER_REACH = 3
TIME_STEPS = 3
LANES = 128
NEAR = (0, PEER_REACH, 2 * PEER_REACH, 2 * PEER_REACH + 1)
FAR = tuple(s for n in range(1, PEER_REACH) for s in (n, PEER_REACH + n))
ORDER = NEAR + FAR
GROUPS = ((0, 4), (4, 4))
MESH = pl.DeviceIdType.MESH
f32, bf16 = jnp.float32, jnp.bfloat16


def dot(a, b):
    return jnp.dot(a, b, preferred_element_type=f32)


def halves(field):
    high = field.astype(bf16)
    return high, (field - high.astype(f32)).astype(bf16)


def stacked_rows(field):
    high = field.astype(bf16).astype(f32)
    both = jnp.concatenate([high, field - high], 0).astype(bf16)
    return jnp.concatenate([both, both], 0)


def row_chunks(rows):
    middle = min(rows, 32)
    return [(0, middle), (middle, rows)] if middle < rows else [(0, rows)]


def halo_ways(slot_number):
    if slot_number < PEER_REACH:
        return "dom", slot_number + 1
    if slot_number < 2 * PEER_REACH:
        return "dom", PEER_REACH - 1 - slot_number
    return "grp", 1 if slot_number == 2 * PEER_REACH else -1


def peer(axis, by):
    place = lax.axis_index(axis)
    count = lax.axis_size(axis)
    if axis == "dom":
        return {axis: lax.rem(place + by + count, count)}, None
    other = place + by
    return {axis: jnp.clip(other, 0, count - 1)}, (other >= 0) & (other < count)


def guarded(condition, action):
    if condition is None:
        action()
    else:
        pl.when(condition)(action)


def hot_of(first, rows, names):
    place = lax.broadcasted_iota(jnp.int32, (rows, names.shape[1]), 0) + first
    return jnp.where(place == names, 1.0, 0.0).astype(bf16)


def steps_kernel(
    names_hbm, x_hbm, faces_hbm, stiff_hbm, own_hbm, other_hbm, star_hbm, near_hbm, far_hbm,
    gains_hbm, element_hbm, slot_hbm, weight_hbm, count_ref, sent_ref,
    out_ref, energy_ref, trace_ref,
    names_ref, faces_ref, stiff_ref, own_ref, other_ref, star_ref, near_ref, far_ref,
    gains_ref, element_ref, slot_ref, weight_ref,
    mats_ref, both, cat, terms, part, tcat, rterm, hs, th,
    hot_own, hot_halo, hot_up, hot_low, hot_rec, wide_weight, msg, held, mine, tabs,
    load_sem, send_sem, recv_sem, table_send, table_recv,
):
    quantities, basis, elements = out_ref.shape
    rows = quantities * basis
    slots = msg.shape[0]
    half = LANES // 2
    upper = msg.shape[1]
    lower = rows - upper
    faces = far_ref.shape[2]
    dims = star_ref.shape[2]
    own_rows = (dims + faces) * basis
    steps = TIME_STEPS
    size = lax.axis_size("dom")
    me = lax.axis_index("dom")
    receivers = trace_ref.shape[2]
    ways = [halo_ways(slot) for slot in range(slots)]

    loads = [
        pltpu.make_async_copy(source, target, load_sem.at[n])
        for n, (source, target) in enumerate(
            [
                (names_hbm, names_ref),
                (x_hbm, out_ref),
                (faces_hbm, faces_ref),
                (stiff_hbm, stiff_ref),
                (own_hbm, own_ref),
                (other_hbm, other_ref),
                (star_hbm, star_ref),
                (near_hbm, near_ref),
                (far_hbm, far_ref),
                (gains_hbm, gains_ref),
                (element_hbm, element_ref),
                (slot_hbm, slot_ref),
                (weight_hbm, weight_ref),
            ]
        )
    ]
    for load in loads:
        load.start()

    barrier = pltpu.get_barrier_semaphore()

    def dom_other(step):
        return {"dom": lax.rem(me + step, size)}

    def greet(step, carry):
        pl.semaphore_signal(barrier, inc=1, device_id=dom_other(step), device_id_type=MESH)
        return carry

    lax.fori_loop(1, size, greet, 0)
    greeted = size - 1
    for axis, by in ways:
        if axis == "grp":
            device, there = peer(axis, by)
            guarded(
                there,
                functools.partial(pl.semaphore_signal, barrier, inc=1, device_id=device, device_id_type=MESH),
            )
            greeted = greeted + there.astype(jnp.int32)

    def copy(step, slot):
        device, there = peer(*ways[slot])
        return (
            pltpu.make_async_remote_copy(
                src_ref=msg.at[slot],
                dst_ref=held.at[step, slot],
                send_sem=send_sem.at[step, slot],
                recv_sem=recv_sem.at[step, slot],
                device_id=device,
                device_id_type=MESH,
            ),
            there,
        )

    def start_slots(step, some):
        for slot in some:
            sent, there = copy(step, slot)
            guarded(there, sent.start)

    def wait_slots(step, some):
        for slot in some:
            sent, _ = copy(step, slot)
            axis, by = ways[slot]
            _, came = peer(axis, -by)
            guarded(came, sent.wait_recv)

    for slot in range(slots):
        axis, by = ways[slot]
        _, came = peer(axis, -by)
        if came is not None:

            @pl.when(jnp.logical_not(came))
            def _(slot=slot):
                for step in range(steps):
                    held[step, slot] = jnp.zeros(held.shape[2:], f32)

    width = 2 * LANES
    loads[0].wait()
    for pair in range(slots // 2):
        even, odd = ORDER[2 * pair], ORDER[2 * pair + 1]
        place = lax.broadcasted_iota(jnp.int32, (1, half), 1)
        first, second = (
            jnp.where(place < sent_ref[0, o], names_ref[o : o + 1, :], -1) for o in (even, odd)
        )
        tile = slice(pair * LANES, (pair + 1) * LANES)
        straight = hot_of(0, elements, jnp.concatenate([first, second], 1))
        crossed = hot_of(0, elements, jnp.concatenate([second, first], 1))
        for again in range(2):
            hot_up[again * elements : (again + 1) * elements, tile] = straight
            hot_low[again * elements : (again + 1) * elements, tile] = crossed

    def paired(action):
        def one(i, carry):
            action(2 * i, 2)
            return carry

        lax.fori_loop(0, quantities // 2, one, 0)
        if quantities % 2:
            action(quantities - 1, 1)

    def split(q, count):
        field = jnp.concatenate([out_ref[q + n] for n in range(count)], 0)
        high, low = halves(field)
        at = pl.ds(pl.multiple_of(q * basis, 16) if not isinstance(q, int) else q * basis, count * basis)
        cat[at, :elements] = high
        cat[at, elements:] = low

    lane = lax.broadcasted_iota(jnp.int32, (upper, LANES), 1)

    def pack(number):
        lanes = slice(number * width, (number + 1) * width)
        up = dot(cat[:upper, :], hot_up[:, lanes])
        low = dot(cat[upper:rows, :], hot_low[:, lanes])
        for pair in range(width // LANES):
            tile = slice(pair * LANES, (pair + 1) * LANES)
            even, odd = ORDER[number * 4 + 2 * pair], ORDER[number * 4 + 2 * pair + 1]
            top, bottom = up[:, tile], low[:, tile]
            here = lane[:lower]
            msg[even, :lower, :] = jnp.where(here < half, top[:lower], bottom)
            msg[odd, :lower, :] = jnp.where(here < half, bottom, top[:lower])
            msg[even, lower:, :] = top[lower:]
            msg[odd, lower:, :] = top[lower:]

    def pack_and_send(step):
        pack(0)
        start_slots(step, NEAR)
        pack(1)
        start_slots(step, FAR)

    loads[1].wait()
    paired(split)
    pl.semaphore_wait(barrier, greeted)
    pack_and_send(0)

    for load in loads[2:]:
        load.wait()
    sources = [(stiff_ref, n, 1.0) for n in range(dims)]
    sources += [(ref, n, -1.0) for ref in (own_ref, other_ref) for n in range(faces)]
    for n in range(0, len(sources), 2):
        some = jnp.concatenate([ref[k] * sign for ref, k, sign in sources[n : n + 2]], 0)
        high = some.astype(bf16).astype(f32)
        low = some - high
        mats_ref[n * basis : n * basis + some.shape[0], :] = jnp.concatenate([high, high, low, low], 1).astype(bf16)

    for f in range(faces):
        names = faces_ref[f : f + 1, :]
        own = hot_of(0, elements, names)
        hot_own[f, :elements, :] = own
        hot_own[f, elements:, :] = own
        for begin, many in GROUPS:
            for n in range(many):
                some = hot_of(elements + ORDER[begin + n] * half, half, names)
                at = (2 * begin + n) * half
                hot_halo[f, at : at + half, :] = some
                hot_halo[f, at + many * half : at + (many + 1) * half, :] = some
    absent = jnp.full((1, LANES - receivers), -1, jnp.int32)
    hot = hot_of(0, elements, jnp.concatenate([element_ref[...], absent], 1))
    slot_row = jnp.concatenate([slot_ref[...], absent], 1).astype(f32)
    wide_weight[...] = jnp.concatenate(
        [weight_ref[...].T, jnp.zeros((basis, LANES - receivers), f32)], 1
    )
    hot_rec[:elements, :] = hot
    hot_rec[elements:, :] = hot
    lane_row = lax.broadcasted_iota(jnp.int32, (1, elements), 1)
    live = lane_row < count_ref[0]

    def store_split(ref, f, q, count, parts, at, gap):
        high, low = halves(jnp.concatenate(parts, 0) if count > 1 else parts[0])
        where = pl.ds(pl.multiple_of(q * basis, 16) if not isinstance(q, int) else q * basis, count * basis)
        wide = high.shape[1]
        ref[f, where, pl.ds(at, wide)] = high
        ref[f, where, pl.ds(at + gap, wide)] = low

    def local_block(at, wide):
        def products(q, count):
            results = [dot(mats_ref[...], both[q + n, :, pl.ds(at, wide)]) for n in range(count)]
            for n in range(count):
                terms[q + n, :, pl.ds(at, wide)] = results[n][:own_rows]
            for f in range(faces):
                low = own_rows + f * basis
                store_split(tcat, f, q, count, [r[low : low + basis] for r in results], at, elements)

        paired(products)

    def window_part(at, wide):
        def gather(f):
            lanes = pl.ds(at, wide)
            picked = dot(tcat[f], hot_own[f, :, lanes])
            rterm[f, :, :, lanes] = picked.reshape(quantities, basis, wide)

        def local(lanes, first, last):
            sums = [jnp.zeros((last - first, LANES), f32) for _ in range(quantities)]
            for q in range(quantities):
                for n in range(dims + faces):
                    ref, k = (star_ref, n) if n < dims else (near_ref, n - dims)
                    term = terms[q, n * basis + first : n * basis + last, lanes]
                    for p in range(quantities):
                        sums[p] = sums[p] + ref[p, q, k : k + 1, lanes] * term
            for p in range(quantities):
                part[p, first:last, lanes] = sums[p]

        work = [
            functools.partial(local, pl.ds(at + sub * LANES, LANES), first, last)
            for sub in range(wide // LANES)
            for first, last in row_chunks(basis)
        ]
        for n in range(max(len(work), faces)):
            if n < faces:
                gather(n)
            if n < len(work):
                work[n]()

    def in_parts(action):
        def one(number, carry):
            action(pl.multiple_of(number * width, width), width)
            return carry

        lax.fori_loop(0, elements // width, one, 0)
        if elements % width:
            action(elements - elements % width, elements % width)

    def halo_terms(step, begin, many):
        cols = many * half
        for pair in range(many // 2):
            tile = slice(pair * LANES, (pair + 1) * LANES)
            at = begin + 2 * pair
            even, odd = held[step, ORDER[at]], held[step, ORDER[at + 1]]
            hs[:upper, tile] = jnp.where(lane < half, even, odd)
            hs[upper:, tile] = pltpu.roll(jnp.where(lane < half, odd, even), half, 1)[: hs.shape[0] - upper]

        def products(q, count):
            results = []
            for n in range(count):
                start = (q + n) * basis
                start = start if isinstance(start, int) else pl.multiple_of(start, 8)
                results.append(dot(mats_ref[own_rows:, :], stacked_rows(hs[pl.ds(start, basis), :cols])))
            for f in range(faces):
                store_split(th, f, q, count, [r[f * basis : (f + 1) * basis] for r in results], 0, cols)

        paired(products)

    def add_halo(f, begin, many, lanes, wide):
        cols = many * half
        late = dot(th[f, :, : 2 * cols], hot_halo[f, 2 * begin * half : 2 * (begin + many) * half, lanes])
        rterm[f, :, :, lanes] = rterm[f, :, :, lanes] + late.reshape(quantities, basis, wide)

    def halo_group(step, begin, many):
        halo_terms(step, begin, many)

        def one_face(f, carry):
            add_halo(f, begin, many, slice(None), elements)
            return carry

        lax.fori_loop(0, faces, one_face, 0)

    def finish_part(at, wide):
        for f in range(faces):
            add_halo(f, *GROUPS[-1], pl.ds(at, wide), wide)
        for sub in range(wide // LANES):
            lanes = pl.ds(at + sub * LANES, LANES)
            alive = at + sub * LANES + lax.broadcasted_iota(jnp.int32, (1, LANES), 1) < count_ref[0]
            for first, last in row_chunks(basis):
                sums = [part[p, first:last, lanes] for p in range(quantities)]
                for f in range(faces):
                    for q in range(quantities):
                        term = rterm[f, q, first:last, lanes]
                        for p in range(quantities):
                            sums[p] = sums[p] + far_ref[p, q, f : f + 1, lanes] * term
                for p in range(quantities):
                    field = out_ref[p, first:last, lanes]
                    out_ref[p, first:last, lanes] = jnp.where(alive, field + sums[p], field)

    def table_copy(step, by, source):
        return pltpu.make_async_remote_copy(
            src_ref=mine.at[step],
            dst_ref=tabs.at[step, source],
            send_sem=table_send.at[step, by],
            recv_sem=table_recv.at[step, source],
            device_id=dom_other(by),
            device_id_type=MESH,
        )

    def one_step(step, carry):
        for q in range(quantities):
            both[q] = stacked_rows(out_ref[q])
        at = 0
        while at < elements:
            wide = min(width, elements - at)
            local_block(at, wide)
            at += wide
        in_parts(window_part)
        for begin, many in GROUPS:
            wait_slots(step, ORDER[begin : begin + many])
            if begin + many < slots:
                halo_group(step, begin, many)
            else:
                halo_terms(step, begin, many)
        in_parts(finish_part)
        paired(split)
        for slot in range(slots):
            sent, there = copy(step, slot)
            guarded(there, sent.wait_send)

        @pl.when(step + 1 < steps)
        def _():
            pack_and_send(step + 1)

        total = jnp.zeros((1, elements), f32)
        picked = dot(cat[...], hot_rec[...])
        for q in range(quantities):
            field = out_ref[q]
            total = total + gains_ref[q : q + 1, :] * jnp.sum(field * field, axis=0, keepdims=True)
            here = picked[q * basis : (q + 1) * basis] * wide_weight[...]
            mine[step, q : q + 1, :] = jnp.sum(here, axis=0, keepdims=True)
        total = jnp.where(live, total, 0.0)
        folded = total[:, :LANES]
        for n in range(1, elements // LANES):
            folded = folded + total[:, n * LANES : (n + 1) * LANES]
        mine[step, quantities : quantities + 1, :] = folded
        mine[step, quantities + 1 : quantities + 2, :] = slot_row

        def start(by, carry):
            table_copy(step, by, me).start()
            return carry

        lax.fori_loop(1, size, start, 0)
        tabs[step, me] = mine[step]
        return carry

    unused = mine.shape[1] - quantities - 2
    for step in range(steps):
        mine[step, quantities + 2 :, :] = jnp.zeros((unused, LANES), f32)
    lax.fori_loop(0, steps, one_step, 0)

    for step in range(steps):

        def finish(by, carry):
            table_copy(step, by, me).wait_send()
            table_copy(step, by, lax.rem(me + by, size)).wait_recv()
            return carry

        lax.fori_loop(1, size, finish, 0)
    wanted = (me * receivers + lax.broadcasted_iota(jnp.int32, (receivers, LANES), 0)).astype(f32)
    hits, values = [], []
    for source in range(size):
        place_row = tabs[0, source, quantities + 1 : quantities + 2, :]
        hits.append(jnp.where(wanted == place_row, 1.0, 0.0).astype(bf16))
        values.append(jnp.concatenate([tabs[step, source] for step in range(steps)], 0))
    hit = jnp.concatenate(hits, 1)
    value = jnp.concatenate(values, 1)
    contract = (((1,), (1,)), ((), ()))
    result = 0.0
    for piece in halves(value):
        result = result + lax.dot_general(piece, hit, contract, preferred_element_type=f32)
    deep = mine.shape[1]
    denominator = float(size * elements * basis * quantities)
    for step in range(steps):
        for q in range(quantities):
            trace_ref[q, step : step + 1, :] = result[step * deep + q : step * deep + q + 1, :]
        row = tabs[step, 0, quantities : quantities + 1, :]
        for source in range(1, size):
            row = row + tabs[step, source, quantities : quantities + 1, :]
        energy_ref[0:1, step : step + 1] = jnp.sum(row, axis=1, keepdims=True) * (0.5 / denominator)


def store_kernel(state_hbm, trace_hbm, energy_hbm, out_hbm, trace_out, energy_out, held, trace, energy, load_sem, store_sem):
    ways = [(state_hbm.at[n], held.at[n], out_hbm.at[n]) for n in range(held.shape[0])]
    ways += [(trace_hbm, trace, trace_out), (energy_hbm, energy, energy_out)]
    loads = [pltpu.make_async_copy(a, b, load_sem.at[n]) for n, (a, b, _) in enumerate(ways)]
    stores = [pltpu.make_async_copy(b, c, store_sem.at[n]) for n, (_, b, c) in enumerate(ways)]
    for load in loads:
        load.start()
    for load, store in zip(loads, stores):
        load.wait()
        store.start()
    for store in stores:
        store.wait()


def per_device(
    element_state,
    stiffness,
    flux_local,
    flux_remote,
    star_matrix,
    face_local,
    face_remote,
    energy_weight,
    face_neighbour,
    element_count,
    send_count,
    send_element,
    receiver_element,
    receiver_slot,
    receiver_weight,
):
    basis, quantities, elements = element_state.shape
    slots, capacity = send_element.shape[1:]
    receivers = receiver_slot.shape[0]
    dimensions, faces = stiffness.shape[0], flux_local.shape[0]
    size = lax.axis_size("dom")
    rows = quantities * basis
    upper = (rows // 2 + 15) // 16 * 16
    group = slots // 2 * capacity
    deep = (quantities + 2 + 7) // 8 * 8

    fields = jnp.transpose(element_state, (1, 0, 2))
    stars = jnp.transpose(star_matrix, (1, 2, 0, 3))
    near = jnp.transpose(face_local, (1, 2, 0, 3))
    far = jnp.transpose(face_remote, (1, 2, 0, 3))

    arrays = (
        send_element[0],
        fields,
        face_neighbour,
        stiffness,
        flux_local,
        flux_remote,
        stars,
        near,
        far,
        energy_weight,
        receiver_element[None, :],
        receiver_slot[None, :],
        receiver_weight.T,
    )
    in_vmem = pl.BlockSpec(memory_space=pltpu.VMEM)
    in_hbm = pl.BlockSpec(memory_space=pltpu.HBM)
    in_smem = pl.BlockSpec(memory_space=pltpu.SMEM)
    vmem = pltpu.VMEM
    state, energy, traces = pl.pallas_call(
        steps_kernel,
        out_shape=(
            jax.ShapeDtypeStruct((quantities, basis, elements), f32),
            jax.ShapeDtypeStruct((1, TIME_STEPS), f32),
            jax.ShapeDtypeStruct((quantities, TIME_STEPS, receivers), f32),
        ),
        in_specs=[in_hbm] * len(arrays) + [in_smem] * 2,
        out_specs=(in_vmem,) * 3,
        scratch_shapes=[
            *[vmem(a.shape, a.dtype) for n, a in enumerate(arrays) if n != 1],
            vmem(((dimensions + 2 * faces) * basis, 4 * basis), bf16),
            vmem((quantities, 4 * basis, elements), bf16),
            vmem((rows, 2 * elements), bf16),
            vmem((quantities, (dimensions + faces) * basis, elements), f32),
            vmem((quantities, basis, elements), f32),
            vmem((faces, rows, 2 * elements), bf16),
            vmem((faces, quantities, basis, elements), f32),
            vmem((rows, group), f32),
            vmem((faces, rows, 2 * group), bf16),
            vmem((faces, 2 * elements, elements), bf16),
            vmem((faces, 2 * slots * capacity, elements), bf16),
            vmem((2 * elements, slots * capacity), bf16),
            vmem((2 * elements, slots * capacity), bf16),
            vmem((2 * elements, LANES), bf16),
            vmem((basis, LANES), f32),
            vmem((slots, upper, LANES), f32),
            vmem((TIME_STEPS, slots, upper, LANES), f32),
            vmem((TIME_STEPS, deep, LANES), f32),
            vmem((TIME_STEPS, size, deep, LANES), f32),
            pltpu.SemaphoreType.DMA((len(arrays),)),
            pltpu.SemaphoreType.DMA((TIME_STEPS, slots)),
            pltpu.SemaphoreType.DMA((TIME_STEPS, slots)),
            pltpu.SemaphoreType.DMA((TIME_STEPS, size)),
            pltpu.SemaphoreType.DMA((TIME_STEPS, size)),
        ],
        compiler_params=pltpu.CompilerParams(
            vmem_limit_bytes=56 << 20, collective_id=0, has_side_effects=True
        ),
        name="steps",
    )(*arrays, element_count, send_count)
    state, traces, energy = pl.pallas_call(
        store_kernel,
        out_shape=tuple(jax.ShapeDtypeStruct(a.shape, f32) for a in (state, traces, energy)),
        in_specs=[in_hbm] * 3,
        out_specs=(in_hbm,) * 3,
        scratch_shapes=[
            *[vmem(a.shape, f32) for a in (state, traces, energy)],
            pltpu.SemaphoreType.DMA((quantities + 2,)),
            pltpu.SemaphoreType.DMA((quantities + 2,)),
        ],
        name="store",
    )(state, traces, energy)
    return (
        jnp.transpose(state, (1, 0, 2)),
        energy,
        jnp.transpose(traces, (1, 0, 2)),
    )


def solution(mesh):
    both = ("grp", "dom")
    return jax.shard_map(
        per_device,
        mesh=mesh,
        in_specs=(
            P(None, None, both),
            P(),
            P(),
            P(),
            P(None, None, None, both),
            P(None, None, None, both),
            P(None, None, None, both),
            P(None, both),
            P(None, both),
            P(both),
            P(both, None),
            P(both, None, None),
            P(both),
            P(both),
            P(None, both),
        ),
        out_specs=(P(None, None, both), P("grp", None), P(None, None, both)),
        check_vma=False,
    )
```

```python
import functools

import jax
import jax.numpy as jnp
from jax import lax
from jax.experimental import pallas as pl
from jax.experimental.pallas import tpu as pltpu
from jax.sharding import PartitionSpec as P

PEER_REACH = 3
TIME_STEPS = 3
LANES = 128
NEAR = (0, PEER_REACH, 2 * PEER_REACH, 2 * PEER_REACH + 1)
FAR = tuple(s for n in range(1, PEER_REACH) for s in (n, PEER_REACH + n))
ORDER = NEAR + FAR
GROUPS = ((0, 4), (4, 4))
MESH = pl.DeviceIdType.MESH
f32, bf16 = jnp.float32, jnp.bfloat16


def dot(a, b):
    return jnp.dot(a, b, preferred_element_type=f32)


def halves(field):
    high = field.astype(bf16)
    return high, (field - high.astype(f32)).astype(bf16)


def stacked_rows(field):
    high = field.astype(bf16).astype(f32)
    both = jnp.concatenate([high, field - high], 0).astype(bf16)
    return jnp.concatenate([both, both], 0)


def row_chunks(rows):
    middle = min(rows, 32)
    return [(0, middle), (middle, rows)] if middle < rows else [(0, rows)]


def halo_ways(slot_number):
    if slot_number < PEER_REACH:
        return "dom", slot_number + 1
    if slot_number < 2 * PEER_REACH:
        return "dom", PEER_REACH - 1 - slot_number
    return "grp", 1 if slot_number == 2 * PEER_REACH else -1


def peer(axis, by):
    place = lax.axis_index(axis)
    count = lax.axis_size(axis)
    if axis == "dom":
        return {axis: lax.rem(place + by + count, count)}, None
    other = place + by
    return {axis: jnp.clip(other, 0, count - 1)}, (other >= 0) & (other < count)


def guarded(condition, action):
    if condition is None:
        action()
    else:
        pl.when(condition)(action)


def hot_of(first, rows, names):
    place = lax.broadcasted_iota(jnp.int32, (rows, names.shape[1]), 0) + first
    return jnp.where(place == names, 1.0, 0.0).astype(bf16)


def steps_kernel(
    names_hbm, x_hbm, faces_hbm, stiff_hbm, own_hbm, other_hbm, star_hbm, near_hbm, far_hbm,
    gains_hbm, element_hbm, slot_hbm, weight_hbm, count_ref, sent_ref,
    out_ref, energy_ref, trace_ref,
    names_ref, faces_ref, stiff_ref, own_ref, other_ref, star_ref, near_ref, far_ref,
    gains_ref, element_ref, slot_ref, weight_ref,
    mats_ref, both, cat, terms, part, tcat, rterm, hs, th,
    hot_own, hot_halo, hot_up, hot_low, hot_rec, wide_weight, msg, held, mine, tabs,
    load_sem, send_sem, recv_sem, table_send, table_recv,
):
    quantities, basis, elements = out_ref.shape
    rows = quantities * basis
    slots = msg.shape[0]
    half = LANES // 2
    upper = msg.shape[1]
    lower = rows - upper
    faces = far_ref.shape[2]
    dims = star_ref.shape[2]
    own_rows = (dims + faces) * basis
    steps = TIME_STEPS
    size = lax.axis_size("dom")
    me = lax.axis_index("dom")
    receivers = trace_ref.shape[2]
    ways = [halo_ways(slot) for slot in range(slots)]

    loads = [
        pltpu.make_async_copy(source, target, load_sem.at[n])
        for n, (source, target) in enumerate(
            [
                (names_hbm, names_ref),
                (x_hbm, out_ref),
                (faces_hbm, faces_ref),
                (stiff_hbm, stiff_ref),
                (own_hbm, own_ref),
                (other_hbm, other_ref),
                (gains_hbm, gains_ref),
                (element_hbm, element_ref),
                (slot_hbm, slot_ref),
                (weight_hbm, weight_ref),
                (star_hbm, star_ref),
                (near_hbm, near_ref),
                (far_hbm, far_ref),
            ]
        )
    ]
    for load in loads[:-3]:
        load.start()

    barrier = pltpu.get_barrier_semaphore()

    def dom_other(step):
        return {"dom": lax.rem(me + step, size)}

    def greet(step, carry):
        pl.semaphore_signal(barrier, inc=1, device_id=dom_other(step), device_id_type=MESH)
        return carry

    lax.fori_loop(1, size, greet, 0)
    greeted = size - 1
    for axis, by in ways:
        if axis == "grp":
            device, there = peer(axis, by)
            guarded(
                there,
                functools.partial(pl.semaphore_signal, barrier, inc=1, device_id=device, device_id_type=MESH),
            )
            greeted = greeted + there.astype(jnp.int32)

    def copy(step, slot):
        device, there = peer(*ways[slot])
        return (
            pltpu.make_async_remote_copy(
                src_ref=msg.at[slot],
                dst_ref=held.at[step, slot],
                send_sem=send_sem.at[step, slot],
                recv_sem=recv_sem.at[step, slot],
                device_id=device,
                device_id_type=MESH,
            ),
            there,
        )

    def start_slots(step, some):
        for slot in some:
            sent, there = copy(step, slot)
            guarded(there, sent.start)

    def wait_slots(step, some):
        for slot in some:
            sent, _ = copy(step, slot)
            axis, by = ways[slot]
            _, came = peer(axis, -by)
            guarded(came, sent.wait_recv)

    for slot in range(slots):
        axis, by = ways[slot]
        _, came = peer(axis, -by)
        if came is not None:

            @pl.when(jnp.logical_not(came))
            def _(slot=slot):
                for step in range(steps):
                    held[step, slot] = jnp.zeros(held.shape[2:], f32)

    width = 2 * LANES
    loads[0].wait()
    for pair in range(slots // 2):
        even, odd = ORDER[2 * pair], ORDER[2 * pair + 1]
        place = lax.broadcasted_iota(jnp.int32, (1, half), 1)
        first, second = (
            jnp.where(place < sent_ref[0, o], names_ref[o : o + 1, :], -1) for o in (even, odd)
        )
        tile = slice(pair * LANES, (pair + 1) * LANES)
        straight = hot_of(0, elements, jnp.concatenate([first, second], 1))
        crossed = hot_of(0, elements, jnp.concatenate([second, first], 1))
        for again in range(2):
            hot_up[again * elements : (again + 1) * elements, tile] = straight
            hot_low[again * elements : (again + 1) * elements, tile] = crossed

    def paired(action):
        def one(i, carry):
            action(2 * i, 2)
            return carry

        lax.fori_loop(0, quantities // 2, one, 0)
        if quantities % 2:
            action(quantities - 1, 1)

    def split(q, count):
        field = jnp.concatenate([out_ref[q + n] for n in range(count)], 0)
        high, low = halves(field)
        at = pl.ds(pl.multiple_of(q * basis, 16) if not isinstance(q, int) else q * basis, count * basis)
        cat[at, :elements] = high
        cat[at, elements:] = low

    lane = lax.broadcasted_iota(jnp.int32, (upper, LANES), 1)

    def pack(number):
        lanes = slice(number * width, (number + 1) * width)
        up = dot(cat[:upper, :], hot_up[:, lanes])
        low = dot(cat[upper:rows, :], hot_low[:, lanes])
        for pair in range(width // LANES):
            tile = slice(pair * LANES, (pair + 1) * LANES)
            even, odd = ORDER[number * 4 + 2 * pair], ORDER[number * 4 + 2 * pair + 1]
            top, bottom = up[:, tile], low[:, tile]
            here = lane[:lower]
            msg[even, :lower, :] = jnp.where(here < half, top[:lower], bottom)
            msg[odd, :lower, :] = jnp.where(here < half, bottom, top[:lower])
            msg[even, lower:, :] = top[lower:]
            msg[odd, lower:, :] = top[lower:]

    def pack_and_send(step):
        pack(0)
        start_slots(step, NEAR)
        pack(1)
        start_slots(step, FAR)

    loads[1].wait()
    for load in loads[-3:]:
        load.start()
    paired(split)
    pack(0)
    pack(1)
    loads[2].wait()

    def build_hot(f):
        names = faces_ref[f : f + 1, :]
        own = hot_of(0, elements, names)
        hot_own[f, :elements, :] = own
        hot_own[f, elements:, :] = own
        for begin, many in GROUPS:
            for n in range(many):
                some = hot_of(elements + ORDER[begin + n] * half, half, names)
                at = (2 * begin + n) * half
                hot_halo[f, at : at + half, :] = some
                hot_halo[f, at + many * half : at + (many + 1) * half, :] = some

    for f in range(faces):
        build_hot(f)
    pl.semaphore_wait(barrier, greeted)
    start_slots(0, ORDER)
    for load in loads[3:]:
        load.wait()
    sources = [(stiff_ref, n, 1.0) for n in range(dims)]
    sources += [(ref, n, -1.0) for ref in (own_ref, other_ref) for n in range(faces)]
    for n in range(0, len(sources), 2):
        some = jnp.concatenate([ref[k] * sign for ref, k, sign in sources[n : n + 2]], 0)
        high = some.astype(bf16).astype(f32)
        low = some - high
        mats_ref[n * basis : n * basis + some.shape[0], :] = jnp.concatenate([high, high, low, low], 1).astype(bf16)

    absent = jnp.full((1, LANES - receivers), -1, jnp.int32)
    hot = hot_of(0, elements, jnp.concatenate([element_ref[...], absent], 1))
    slot_row = jnp.concatenate([slot_ref[...], absent], 1).astype(f32)
    wide_weight[...] = jnp.concatenate(
        [weight_ref[...].T, jnp.zeros((basis, LANES - receivers), f32)], 1
    )
    hot_rec[:elements, :] = hot
    hot_rec[elements:, :] = hot
    lane_row = lax.broadcasted_iota(jnp.int32, (1, elements), 1)
    live = lane_row < count_ref[0]

    def store_split(ref, f, q, count, parts, at, gap):
        high, low = halves(jnp.concatenate(parts, 0) if count > 1 else parts[0])
        where = pl.ds(pl.multiple_of(q * basis, 16) if not isinstance(q, int) else q * basis, count * basis)
        wide = high.shape[1]
        ref[f, where, pl.ds(at, wide)] = high
        ref[f, where, pl.ds(at + gap, wide)] = low

    def local_block(at, wide):
        def products(q, count):
            results = [dot(mats_ref[...], both[q + n, :, pl.ds(at, wide)]) for n in range(count)]
            for n in range(count):
                terms[q + n, :, pl.ds(at, wide)] = results[n][:own_rows]
            for f in range(faces):
                low = own_rows + f * basis
                store_split(tcat, f, q, count, [r[low : low + basis] for r in results], at, elements)

        paired(products)

    def window_part(at, wide):
        def gather(f):
            lanes = pl.ds(at, wide)
            picked = dot(tcat[f], hot_own[f, :, lanes])
            rterm[f, :, :, lanes] = picked.reshape(quantities, basis, wide)

        def local(lanes, first, last):
            sums = [jnp.zeros((last - first, LANES), f32) for _ in range(quantities)]
            for q in range(quantities):
                for n in range(dims + faces):
                    ref, k = (star_ref, n) if n < dims else (near_ref, n - dims)
                    term = terms[q, n * basis + first : n * basis + last, lanes]
                    for p in range(quantities):
                        sums[p] = sums[p] + ref[p, q, k : k + 1, lanes] * term
            for p in range(quantities):
                part[p, first:last, lanes] = sums[p]

        work = [
            functools.partial(local, pl.ds(at + sub * LANES, LANES), first, last)
            for sub in range(wide // LANES)
            for first, last in row_chunks(basis)
        ]
        for n in range(max(len(work), faces)):
            if n < faces:
                gather(n)
            if n < len(work):
                work[n]()

    def in_parts(action):
        def one(number, carry):
            action(pl.multiple_of(number * width, width), width)
            return carry

        lax.fori_loop(0, elements // width, one, 0)
        if elements % width:
            action(elements - elements % width, elements % width)

    def halo_terms(step, begin, many):
        cols = many * half
        for pair in range(many // 2):
            tile = slice(pair * LANES, (pair + 1) * LANES)
            at = begin + 2 * pair
            even, odd = held[step, ORDER[at]], held[step, ORDER[at + 1]]
            hs[:upper, tile] = jnp.where(lane < half, even, odd)
            hs[upper:, tile] = pltpu.roll(jnp.where(lane < half, odd, even), half, 1)[: hs.shape[0] - upper]

        def products(q, count):
            results = []
            for n in range(count):
                start = (q + n) * basis
                start = start if isinstance(start, int) else pl.multiple_of(start, 8)
                results.append(dot(mats_ref[own_rows:, :], stacked_rows(hs[pl.ds(start, basis), :cols])))
            for f in range(faces):
                store_split(th, f, q, count, [r[f * basis : (f + 1) * basis] for r in results], 0, cols)

        paired(products)

    def add_halo(f, begin, many, lanes, wide):
        cols = many * half
        late = dot(th[f, :, : 2 * cols], hot_halo[f, 2 * begin * half : 2 * (begin + many) * half, lanes])
        rterm[f, :, :, lanes] = rterm[f, :, :, lanes] + late.reshape(quantities, basis, wide)

    def halo_group(step, begin, many):
        halo_terms(step, begin, many)

        def one_face(f, carry):
            add_halo(f, begin, many, slice(None), elements)
            return carry

        lax.fori_loop(0, faces, one_face, 0)

    def finish_part(at, wide):
        for f in range(faces):
            add_halo(f, *GROUPS[-1], pl.ds(at, wide), wide)
        for sub in range(wide // LANES):
            lanes = pl.ds(at + sub * LANES, LANES)
            alive = at + sub * LANES + lax.broadcasted_iota(jnp.int32, (1, LANES), 1) < count_ref[0]
            for first, last in row_chunks(basis):
                sums = [part[p, first:last, lanes] for p in range(quantities)]
                for f in range(faces):
                    for q in range(quantities):
                        term = rterm[f, q, first:last, lanes]
                        for p in range(quantities):
                            sums[p] = sums[p] + far_ref[p, q, f : f + 1, lanes] * term
                for p in range(quantities):
                    field = out_ref[p, first:last, lanes]
                    out_ref[p, first:last, lanes] = jnp.where(alive, field + sums[p], field)

    def table_copy(step, by, source):
        return pltpu.make_async_remote_copy(
            src_ref=mine.at[step],
            dst_ref=tabs.at[step, source],
            send_sem=table_send.at[step, by],
            recv_sem=table_recv.at[step, source],
            device_id=dom_other(by),
            device_id_type=MESH,
        )

    def one_step(step, carry):
        for q in range(quantities):
            both[q] = stacked_rows(out_ref[q])
        at = 0
        while at < elements:
            wide = min(width, elements - at)
            local_block(at, wide)
            at += wide
        in_parts(window_part)
        for begin, many in GROUPS:
            wait_slots(step, ORDER[begin : begin + many])
            if begin + many < slots:
                halo_group(step, begin, many)
            else:
                halo_terms(step, begin, many)
        in_parts(finish_part)
        paired(split)
        for slot in range(slots):
            sent, there = copy(step, slot)
            guarded(there, sent.wait_send)

        @pl.when(step + 1 < steps)
        def _():
            pack_and_send(step + 1)

        total = jnp.zeros((1, elements), f32)
        picked = dot(cat[...], hot_rec[...])
        for q in range(quantities):
            field = out_ref[q]
            total = total + gains_ref[q : q + 1, :] * jnp.sum(field * field, axis=0, keepdims=True)
            here = picked[q * basis : (q + 1) * basis] * wide_weight[...]
            mine[step, q : q + 1, :] = jnp.sum(here, axis=0, keepdims=True)
        total = jnp.where(live, total, 0.0)
        folded = total[:, :LANES]
        for n in range(1, elements // LANES):
            folded = folded + total[:, n * LANES : (n + 1) * LANES]
        mine[step, quantities : quantities + 1, :] = folded
        mine[step, quantities + 1 : quantities + 2, :] = slot_row

        def start(by, carry):
            table_copy(step, by, me).start()
            return carry

        lax.fori_loop(1, size, start, 0)
        tabs[step, me] = mine[step]
        return carry

    unused = mine.shape[1] - quantities - 2
    for step in range(steps):
        mine[step, quantities + 2 :, :] = jnp.zeros((unused, LANES), f32)
    lax.fori_loop(0, steps, one_step, 0)

    for step in range(steps):

        def finish(by, carry):
            table_copy(step, by, me).wait_send()
            table_copy(step, by, lax.rem(me + by, size)).wait_recv()
            return carry

        lax.fori_loop(1, size, finish, 0)
    wanted = (me * receivers + lax.broadcasted_iota(jnp.int32, (receivers, LANES), 0)).astype(f32)
    hits, values = [], []
    for source in range(size):
        place_row = tabs[0, source, quantities + 1 : quantities + 2, :]
        hits.append(jnp.where(wanted == place_row, 1.0, 0.0).astype(bf16))
        values.append(jnp.concatenate([tabs[step, source] for step in range(steps)], 0))
    hit = jnp.concatenate(hits, 1)
    value = jnp.concatenate(values, 1)
    contract = (((1,), (1,)), ((), ()))
    result = 0.0
    for piece in halves(value):
        result = result + lax.dot_general(piece, hit, contract, preferred_element_type=f32)
    deep = mine.shape[1]
    denominator = float(size * elements * basis * quantities)
    for step in range(steps):
        for q in range(quantities):
            trace_ref[q, step : step + 1, :] = result[step * deep + q : step * deep + q + 1, :]
        row = tabs[step, 0, quantities : quantities + 1, :]
        for source in range(1, size):
            row = row + tabs[step, source, quantities : quantities + 1, :]
        energy_ref[0:1, step : step + 1] = jnp.sum(row, axis=1, keepdims=True) * (0.5 / denominator)


def store_kernel(state_hbm, trace_hbm, energy_hbm, out_hbm, trace_out, energy_out, held, trace, energy, load_sem, store_sem):
    ways = [(state_hbm.at[n], held.at[n], out_hbm.at[n]) for n in range(held.shape[0])]
    ways += [(trace_hbm, trace, trace_out), (energy_hbm, energy, energy_out)]
    loads = [pltpu.make_async_copy(a, b, load_sem.at[n]) for n, (a, b, _) in enumerate(ways)]
    stores = [pltpu.make_async_copy(b, c, store_sem.at[n]) for n, (_, b, c) in enumerate(ways)]
    for load in loads:
        load.start()
    for load, store in zip(loads, stores):
        load.wait()
        store.start()
    for store in stores:
        store.wait()


def per_device(
    element_state,
    stiffness,
    flux_local,
    flux_remote,
    star_matrix,
    face_local,
    face_remote,
    energy_weight,
    face_neighbour,
    element_count,
    send_count,
    send_element,
    receiver_element,
    receiver_slot,
    receiver_weight,
):
    basis, quantities, elements = element_state.shape
    slots, capacity = send_element.shape[1:]
    receivers = receiver_slot.shape[0]
    dimensions, faces = stiffness.shape[0], flux_local.shape[0]
    size = lax.axis_size("dom")
    rows = quantities * basis
    upper = (rows // 2 + 15) // 16 * 16
    group = slots // 2 * capacity
    deep = (quantities + 2 + 7) // 8 * 8

    fields = jnp.transpose(element_state, (1, 0, 2))
    stars = jnp.transpose(star_matrix, (1, 2, 0, 3))
    near = jnp.transpose(face_local, (1, 2, 0, 3))
    far = jnp.transpose(face_remote, (1, 2, 0, 3))

    arrays = (
        send_element[0],
        fields,
        face_neighbour,
        stiffness,
        flux_local,
        flux_remote,
        stars,
        near,
        far,
        energy_weight,
        receiver_element[None, :],
        receiver_slot[None, :],
        receiver_weight.T,
    )
    in_vmem = pl.BlockSpec(memory_space=pltpu.VMEM)
    in_hbm = pl.BlockSpec(memory_space=pltpu.HBM)
    in_smem = pl.BlockSpec(memory_space=pltpu.SMEM)
    vmem = pltpu.VMEM
    state, energy, traces = pl.pallas_call(
        steps_kernel,
        out_shape=(
            jax.ShapeDtypeStruct((quantities, basis, elements), f32),
            jax.ShapeDtypeStruct((1, TIME_STEPS), f32),
            jax.ShapeDtypeStruct((quantities, TIME_STEPS, receivers), f32),
        ),
        in_specs=[in_hbm] * len(arrays) + [in_smem] * 2,
        out_specs=(in_vmem,) * 3,
        scratch_shapes=[
            *[vmem(a.shape, a.dtype) for n, a in enumerate(arrays) if n != 1],
            vmem(((dimensions + 2 * faces) * basis, 4 * basis), bf16),
            vmem((quantities, 4 * basis, elements), bf16),
            vmem((rows, 2 * elements), bf16),
            vmem((quantities, (dimensions + faces) * basis, elements), f32),
            vmem((quantities, basis, elements), f32),
            vmem((faces, rows, 2 * elements), bf16),
            vmem((faces, quantities, basis, elements), f32),
            vmem((rows, group), f32),
            vmem((faces, rows, 2 * group), bf16),
            vmem((faces, 2 * elements, elements), bf16),
            vmem((faces, 2 * slots * capacity, elements), bf16),
            vmem((2 * elements, slots * capacity), bf16),
            vmem((2 * elements, slots * capacity), bf16),
            vmem((2 * elements, LANES), bf16),
            vmem((basis, LANES), f32),
            vmem((slots, upper, LANES), f32),
            vmem((TIME_STEPS, slots, upper, LANES), f32),
            vmem((TIME_STEPS, deep, LANES), f32),
            vmem((TIME_STEPS, size, deep, LANES), f32),
            pltpu.SemaphoreType.DMA((len(arrays),)),
            pltpu.SemaphoreType.DMA((TIME_STEPS, slots)),
            pltpu.SemaphoreType.DMA((TIME_STEPS, slots)),
            pltpu.SemaphoreType.DMA((TIME_STEPS, size)),
            pltpu.SemaphoreType.DMA((TIME_STEPS, size)),
        ],
        compiler_params=pltpu.CompilerParams(
            vmem_limit_bytes=56 << 20, collective_id=0, has_side_effects=True
        ),
        name="steps",
    )(*arrays, element_count, send_count)
    state, traces, energy = pl.pallas_call(
        store_kernel,
        out_shape=tuple(jax.ShapeDtypeStruct(a.shape, f32) for a in (state, traces, energy)),
        in_specs=[in_hbm] * 3,
        out_specs=(in_hbm,) * 3,
        scratch_shapes=[
            *[vmem(a.shape, f32) for a in (state, traces, energy)],
            pltpu.SemaphoreType.DMA((quantities + 2,)),
            pltpu.SemaphoreType.DMA((quantities + 2,)),
        ],
        name="store",
    )(state, traces, energy)
    return (
        jnp.transpose(state, (1, 0, 2)),
        energy,
        jnp.transpose(traces, (1, 0, 2)),
    )


def solution(mesh):
    both = ("grp", "dom")
    return jax.shard_map(
        per_device,
        mesh=mesh,
        in_specs=(
            P(None, None, both),
            P(),
            P(),
            P(),
            P(None, None, None, both),
            P(None, None, None, both),
            P(None, None, None, both),
            P(None, both),
            P(None, both),
            P(both),
            P(both, None),
            P(both, None, None),
            P(both),
            P(both),
            P(None, both),
        ),
        out_specs=(P(None, None, both), P("grp", None), P(None, None, both)),
        check_vma=False,
    )
```
